256 devices in a mesh: groups: 2 (over y), seq: 16 (over z), head: 8 (over x, core).
Axes of the slice: x: 4, y: 2, z: 16, core: 2. Of those that a mesh axis runs over, the one named last changes fastest.
The devices are a block of a 4x16x16 slice.
Arguments:
- residual: bfloat16 [16384, 2560], P(('groups', 'seq'), 'head'), parts along dimension 0, may hold values from -6 to 6
- x_in: bfloat16 [16384, 5120], P(('groups', 'seq'), 'head'), parts along dimension 0, may hold values from -6 to 6
- bc_in: bfloat16 [16384, 256], P(('groups', 'seq')), parts along dimension 0, may hold values from -1.5 to 1.5
- z_in: bfloat16 [16384, 5120], P(('groups', 'seq'), 'head'), parts along dimension 0, may hold values from -6 to 6
- dt_raw: float32 [80, 16384], P('head', ('groups', 'seq')), parts along dimension 1, may hold values from -5 to 5
- dt_bias: float32 [80], P('head'), may hold values from -3 to 0
- decay_rate: float32 [80], P('head'), may hold values from 0.0003 to 0.15
- d_skip: float32 [80], P('head'), may hold values from 1 to 4
- conv_x_weight: bfloat16 [4, 5120], P(None, 'head'), may hold values from -3 to 3
- conv_x_bias: bfloat16 [5120], P('head'), may hold values from -3 to 3
- conv_bc_weight: bfloat16 [4, 256], replicated, may hold values from -3 to 3
- conv_bc_bias: bfloat16 [256], replicated, may hold values from -3 to 3
- norm_gain: bfloat16 [5120], P('head'), may hold values from 0.5 to 1.5
- out_weight: bfloat16 [5120, 2560], P('head'), may hold values from -0.078125 to 0.078125
- final_gain: bfloat16 [2560], replicated, may hold values from 0.5 to 1.5
- lm_weight: bfloat16 [2560, 25600], P('seq', 'head'), may hold values from -15.811388 to 15.811388
- targets: int32 [16384], P(('groups', 'seq')), parts along dimension 0, may hold values from 0 to 25599
- doc_lengths: int32 [32], P('groups'), parts along dimension 0, may hold values from 1 to 1536, as said below
Outputs:
- block_out: bfloat16 [16384, 2560], P(('groups', 'seq'), 'head'), parts along dimension 0
- doc_loss: float32 [32], P('groups'), parts along dimension 0
The draws below stay inside these ranges and needn't reach their ends.
There are 2 independent parts, one for each index of `groups`. The reference program is written for one: setup_inputs(seed, part) draws one part's arguments, and reference() takes and returns one part's arrays. A program takes and returns all parts, laid end to end along the dimension named above; an argument that names none is the same for every part. Nothing has to cross between parts.
Inputs may be any that keep to these rules, and one draw needn't show every extreme that they name: `doc_lengths`: the lengths of a group's 16 documents, in the order in which they are packed into its 8192 tokens; they sum to 8192.
All inputs are finite; a program needn't handle non-finite values.
Results may differ from the reference program's by a relative error of at most 0.00145.
The reference program's roundings to bfloat16 on the way count: a program that leaves them out, or rounds other values in their place, can miss the bound.
Values may be sent and summed in bfloat16 or wider, within the bound.
No kernel may reach another device: no remote copies, remote signals or barrier semaphores. Data moves between devices by JAX's collectives and lax.ppermute only.
A program may use at most 128 MiB of HBM per device.

```python
import math
import jax
import jax.numpy as jnp
import numpy as np
from jax import lax

D = 2560
HEADS = 80
HEAD_SIZE = 64
STATE = 128
KERNEL = 4
VOCAB = 25600
SPAN = 256
TOK_DEV = 512
INNER = 5120
TOKENS = 8192
DOCS = 16
N_SEQ = 16


def draw_lm_weight(key, part):
    entries = jax.random.truncated_normal(jax.random.fold_in(key, 11), -5.0, 5.0, (D, VOCAB), jnp.float32) * (3.0 / math.sqrt(D))
    return entries.astype(jnp.bfloat16)


def draw_doc_lengths(key, part):
    longest = 3 * TOK_DEV
    rest = TOKENS - longest
    others = DOCS - 1
    spacing = rest // others
    jitter = jax.random.randint(jax.random.fold_in(key, 21), (others - 1,), 0, spacing, jnp.int32)
    cuts = (jnp.arange(1, others, dtype=jnp.int32) * spacing + jitter).astype(jnp.int32)
    edges = jnp.concatenate([jnp.zeros((1,), jnp.int32), cuts, jnp.full((1,), rest, jnp.int32)])
    pieces = (edges[1:] - edges[:-1]).astype(jnp.int32)
    joined = jnp.concatenate([pieces, jnp.full((1,), longest, jnp.int32)])
    place = jax.random.randint(jax.random.fold_in(key, 22), (), 0, DOCS, jnp.int32)
    order = jnp.arange(DOCS, dtype=jnp.int32)
    index = jnp.where(order < place, order, jnp.where(order == place, others, order - 1)).astype(jnp.int32)
    return joined[index]


def plant(array, own_key, least, largest):
    longest = array.shape.index(max(array.shape))
    spots = []
    for shift in (0, 1):
        where = [jax.random.randint(jax.random.fold_in(own_key, axis), (), 0, length) for axis, length in enumerate(array.shape)]
        where[longest] = (where[longest] + shift) % array.shape[longest]
        spots.append(tuple(where))
    return array.at[spots[0]].set(least).at[spots[1]].set(largest)


def steps_of(own_key, shape, split, low, high):
    gain = 1.0
    for axis_at, blocks in split:
        draws = jax.random.uniform(jax.random.fold_in(jax.random.fold_in(own_key, 6), axis_at), (blocks,), jnp.float32, low / len(split), high / len(split))
        gain = gain * jnp.repeat(jnp.exp(draws), shape[axis_at] // blocks).reshape((-1,) + (1,) * (len(shape) - 1 - axis_at))
    return gain


def rank_bounds(amount, lean):
    portions = [(1 << 20) // math.isqrt(standing ** lean) + 1 for standing in range(1, amount + 1)]
    width = 1 + sum(portions) // (1 << 30)
    return np.cumsum(np.array([max(1, weight // width) for weight in portions]))


def skewed_ids(rng, shape, number_of, slope):
    listing = rank_bounds(number_of, slope)
    lot = jax.random.randint(jax.random.fold_in(rng, 1), shape, 0, int(listing[number_of - 1]))
    rank = jnp.searchsorted(jnp.asarray(listing, jnp.int32), lot, side="right")
    return jax.random.permutation(jax.random.fold_in(rng, 2), number_of)[rank].astype(jnp.int32)


def gaussian(rng, dims, width, limit, shards=(), kind=jnp.bfloat16):
    result = jax.random.normal(rng, dims, jnp.float32) * width
    if len(shards) > 0:
        result = steps_of(rng, dims, shards, -0.22, 0.18) * result
    return jnp.clip(result, min=-limit, max=limit).astype(kind)


def setup_inputs(seed: int = 0, part: int = 0) -> dict:
    arg_keys = jax.random.split(jax.random.key(seed), 19)
    part_splits = jax.random.split(jax.random.fold_in(arg_keys[18], part), 19)
    return {
        "residual": gaussian(part_splits[0], (TOKENS, D), 1.0, 6.0, ((0, 16), (1, 8))),
        "x_in": gaussian(part_splits[1], (TOKENS, INNER), 1.0, 6.0, ((0, 16), (1, 8))),
        "bc_in": gaussian(part_splits[2], (TOKENS, 2 * STATE), 0.25, 1.5, ((0, 16),)),
        "z_in": gaussian(part_splits[3], (TOKENS, INNER), 1.0, 6.0, ((0, 16), (1, 8))),
        "dt_raw": gaussian(part_splits[4], (HEADS, TOKENS), 1.0, 5.0, ((0, 8), (1, 16)), jnp.float32),
        "dt_bias": jnp.clip(-3.0 + 3.0 * jax.random.uniform(arg_keys[5], (HEADS,), jnp.float32) ** steps_of(arg_keys[5], (HEADS,), ((0, 8),), -0.2, 0.2), -3.0, 0.0),
        "decay_rate": jnp.clip(jnp.exp(math.log(0.15) - 6.214608 * jax.random.uniform(arg_keys[6], (HEADS,), jnp.float32) ** steps_of(arg_keys[6], (HEADS,), ((0, 8),), -0.2, 0.2)), 0.0003, 0.15),
        "d_skip": jnp.clip(1.0 + 3.0 * jax.random.uniform(arg_keys[7], (HEADS,), jnp.float32) ** steps_of(arg_keys[7], (HEADS,), ((0, 8),), -0.2, 0.2), 1.0, 4.0),
        "conv_x_weight": gaussian(arg_keys[8], (KERNEL, INNER), KERNEL ** -0.5, 3.0, ((1, 8),)),
        "conv_x_bias": gaussian(arg_keys[9], (INNER,), 0.5, 3.0, ((0, 8),)),
        "conv_bc_weight": gaussian(arg_keys[10], (KERNEL, 2 * STATE), KERNEL ** -0.5, 3.0),
        "conv_bc_bias": gaussian(arg_keys[11], (2 * STATE,), 0.5, 3.0),
        "norm_gain": jnp.clip(1.0 + 0.1 * jax.random.normal(arg_keys[12], (INNER,), jnp.float32), 0.5, 1.5).astype(jnp.bfloat16),
        "out_weight": gaussian(arg_keys[13], (INNER, D), INNER ** -0.5, 0.078125, ((0, 8),)),
        "final_gain": jnp.clip(1.0 + 0.1 * jax.random.normal(arg_keys[14], (D,), jnp.float32), 0.5, 1.5).astype(jnp.bfloat16),
        "lm_weight": draw_lm_weight(jax.random.fold_in(arg_keys[18], 71), part),
        "targets": plant(skewed_ids(part_splits[16], (TOKENS,), VOCAB, 2), jax.random.fold_in(part_splits[16], 3), 0, VOCAB - 1).astype(jnp.int32),
        "doc_lengths": draw_doc_lengths(jax.random.fold_in(jax.random.fold_in(arg_keys[18], part), 71), part),
    }


EPSILON = 1e-05
HIGH = lax.Precision.HIGHEST

def document_of(positions, doc_lengths):
    starts = jnp.cumsum(doc_lengths) - doc_lengths
    return lax.optimization_barrier(jnp.sum((positions[:, None] >= starts[None, :]).astype(jnp.int32), axis=1)) - 1

def causal_conv(signal, rim_rows, weight, bias, positions, doc_ids, doc_lengths):
    length = signal.shape[0]
    taps = weight.shape[0]
    joined = jnp.concatenate([rim_rows, signal], axis=0).astype(jnp.float32)
    total = jnp.zeros(signal.shape, jnp.float32) + bias.astype(jnp.float32)[None, :]
    for offset in range(taps):
        lag = taps - 1 - offset
        source = document_of(positions - lag, doc_lengths)
        same = (source == doc_ids).astype(jnp.float32)
        total = total + weight[offset].astype(jnp.float32)[None, :] * joined[offset:offset + length] * same[:, None]
    return jax.nn.silu(total).astype(jnp.bfloat16)

def span_step(state, pieces, rates):
    signal, bmat, cmat, steps, doc_ids, doc_prev = pieces
    signal = signal.astype(jnp.float32)
    bmat = bmat.astype(jnp.float32)
    cmat = cmat.astype(jnp.float32)
    climb = jnp.cumsum(steps * rates[:, None], axis=1)
    extent = doc_ids.shape[0]
    order = jnp.arange(extent, dtype=jnp.int32)
    inside = (doc_ids[:, None] == doc_ids[None, :]) & (order[:, None] >= order[None, :])
    gap = climb[:, :, None] - climb[:, None, :]
    decay = jnp.where(inside[None], jnp.exp(-jnp.where(inside[None], gap, 0.0)), 0.0)
    scores = jnp.dot(cmat, bmat.T, precision=HIGH)
    weights = decay * scores[None] * steps[:, None, :]
    output = jnp.einsum('hts,shp->thp', weights, signal, precision=HIGH)
    carried = (doc_ids == doc_prev).astype(jnp.float32)
    entry = jnp.exp(-climb) * carried[None, :]
    output = output + jnp.einsum('tn,hpn->thp', cmat, state, precision=HIGH) * entry.T[:, :, None]
    last = doc_ids[extent - 1]
    tail = jnp.exp(climb - climb[:, extent - 1:]) * (doc_ids == last).astype(jnp.float32)[None, :] * steps
    kept = jnp.exp(-climb[:, extent - 1]) * (last == doc_prev).astype(jnp.float32)
    fresh = jnp.einsum('hs,shp,sn->hpn', tail, signal, bmat, precision=HIGH)
    return (kept[:, None, None] * state + fresh, output)

def reference(residual, x_in, bc_in, z_in, dt_raw, dt_bias, decay_rate, d_skip, conv_x_weight, conv_x_bias, conv_bc_weight, conv_bc_bias, norm_gain, out_weight, final_gain, lm_weight, targets, doc_lengths):
    positions = jnp.arange(TOKENS, dtype=jnp.int32)
    doc_ids = document_of(positions, doc_lengths)
    margin = KERNEL - 1
    signal = causal_conv(x_in, jnp.zeros((margin, INNER), jnp.bfloat16), conv_x_weight, conv_x_bias, positions, doc_ids, doc_lengths)
    keys_queries = causal_conv(bc_in, jnp.zeros((margin, 2 * STATE), jnp.bfloat16), conv_bc_weight, conv_bc_bias, positions, doc_ids, doc_lengths)
    steps = jax.nn.softplus(dt_raw + dt_bias[:, None])
    blocks = TOKENS // SPAN
    block_starts = jnp.arange(blocks, dtype=jnp.int32) * SPAN
    pieces = (signal.reshape(blocks, SPAN, HEADS, HEAD_SIZE), keys_queries[:, :STATE].reshape(blocks, SPAN, STATE), keys_queries[:, STATE:].reshape(blocks, SPAN, STATE), steps.reshape(HEADS, blocks, SPAN).transpose(1, 0, 2), doc_ids.reshape(blocks, SPAN), document_of(block_starts - 1, doc_lengths))

    def advance(state, piece):
        return span_step(state, piece, decay_rate)
    ignored, outputs = lax.scan(advance, jnp.zeros((HEADS, HEAD_SIZE, STATE), jnp.float32), pieces)
    mixed = outputs.reshape(TOKENS, HEADS, HEAD_SIZE) + d_skip[None, :, None] * signal.reshape(TOKENS, HEADS, HEAD_SIZE).astype(jnp.float32)
    gated = mixed.reshape(TOKENS, INNER) * jax.nn.silu(z_in.astype(jnp.float32))
    scale = lax.rsqrt(lax.optimization_barrier(jnp.sum(gated * gated, axis=1)) / INNER + EPSILON)
    normed = (gated * scale[:, None] * norm_gain.astype(jnp.float32)[None, :]).astype(jnp.bfloat16)
    projected = jnp.dot(normed, out_weight, preferred_element_type=jnp.float32)
    block_out = (residual.astype(jnp.float32) + projected).astype(jnp.bfloat16)
    widened = block_out.astype(jnp.float32)
    final_scale = lax.rsqrt(lax.optimization_barrier(jnp.sum(widened * widened, axis=1)) / D + EPSILON)
    hidden = (widened * final_scale[:, None] * final_gain.astype(jnp.float32)[None, :]).astype(jnp.bfloat16)

    def token_loss(piece):
        hidden_rows, target_rows = piece
        logits = jnp.dot(hidden_rows, lm_weight, preferred_element_type=jnp.float32)
        peak = lax.optimization_barrier(jnp.max(logits, axis=1))
        total = lax.optimization_barrier(jnp.sum(jnp.exp(logits - peak[:, None]), axis=1))
        column = jnp.arange(VOCAB, dtype=jnp.int32)
        picked = lax.optimization_barrier(jnp.sum(jnp.where(column[None, :] == target_rows[:, None], logits, 0.0), axis=1))
        return peak + jnp.log(total) - picked
    losses = lax.map(token_loss, (hidden.reshape(N_SEQ, TOK_DEV, D), targets.reshape(N_SEQ, TOK_DEV))).reshape(TOKENS)
    member = (doc_ids[:, None] == jnp.arange(DOCS, dtype=jnp.int32)[None, :]).astype(jnp.float32)
    sums = jnp.dot(losses, member, precision=HIGH)
    return (block_out, sums / doc_lengths.astype(jnp.float32))
```

```python
import functools

import jax
import jax.numpy as jnp
from jax import lax
from jax.experimental import pallas as pl
from jax.experimental.pallas import tpu as pltpu
from jax.sharding import Mesh
from jax.sharding import PartitionSpec as P

STATE = 128
HEAD_SIZE = 64
KERNEL = 4
LONGEST = 1536
EPSILON = 1e-05
LANES = 128
RIM = 8
NEG = -1e30
F32 = jnp.float32
BF16 = jnp.bfloat16

SMEM = pl.BlockSpec(memory_space=pltpu.SMEM)
HEADS_AXES = ("x", "core")


def dot(a, b, ca=1, cb=0):
    return lax.dot_general(a, b, (((ca,), (cb,)), ((), ())), preferred_element_type=F32)


def in_two(value):
    high = value.astype(BF16)
    return high, (value - high.astype(F32)).astype(BF16)


def in_three(value):
    high = value.astype(BF16)
    rest = value - high.astype(F32)
    middle = rest.astype(BF16)
    return high, middle, (rest - middle.astype(F32)).astype(BF16)


def silu(value):
    return value * jax.nn.sigmoid(value)


def starts_of(lens):
    start = jnp.int32(0)
    for d in range(lens.shape[0]):
        yield start
        start = start + lens[d]


def own_starts(lens, offset, length):
    pos = offset + lax.broadcasted_iota(jnp.int32, (length, LANES), 0)
    found = jnp.zeros((length, LANES), jnp.int32)
    for start in starts_of(lens):
        found = jnp.where(pos >= start, start, found)
    return pos, found


def pair_of(cols, at):
    lane = lax.broadcasted_iota(jnp.int32, (cols.shape[0], LANES), 1)
    return jnp.where(lane < HEAD_SIZE, cols[:, at : at + 1], cols[:, at + 1 : at + 2])


def front_kernel(
    lens, offset_ref, x_ref, xr_ref, bc_ref, bcr_ref, dt_ref, hp_ref, cw_ref, cb_ref, bw_ref, bb_ref,
    val_ref, kq_ref, cols_ref, rows_ref, e_ref, d_ref, xs, bs, rs,
):
    length, width = x_ref.shape
    heads = dt_ref.shape[0]
    offset = offset_ref[0]
    pos, found = own_starts(lens, offset, length)
    depth = pos - found
    last_start = jnp.int32(0)
    first_here = jnp.int32(2**30)
    for start in starts_of(lens):
        last_start = jnp.where(start <= offset + length - 1, start, last_start)
        first_here = jnp.where(start >= offset, jnp.minimum(first_here, start), first_here)

    bs[:RIM] = bcr_ref[...].astype(F32)
    bs[RIM:] = bc_ref[...].astype(F32)
    xs[:RIM] = xr_ref[...].astype(F32)
    xs[RIM:] = x_ref[...].astype(F32)

    def conv(buf, w_ref, b_ref, at):
        sl = slice(at, at + LANES)
        total = jnp.zeros((length, LANES), F32) + b_ref[:, sl].astype(F32)
        for k in range(KERNEL):
            lag = KERNEL - 1 - k
            tap = w_ref[k : k + 1, sl].astype(F32) * buf[RIM - lag : RIM - lag + length, sl]
            total = total + (jnp.where(depth >= lag, tap, 0.0) if lag else tap)
        return silu(total).astype(BF16)

    for at in range(0, 2 * STATE, LANES):
        kq_ref[:, at : at + LANES] = conv(bs, bw_ref, bb_ref, at)

    hp = hp_ref[...]
    raw = dt_ref[...] + hp[:, 0:1]
    steps = jnp.maximum(raw, 0.0) + jnp.log1p(jnp.exp(-jnp.abs(raw)))
    rates = steps * hp[:, 1:2]
    upper = (
        lax.broadcasted_iota(jnp.int32, (length, length), 0)
        <= lax.broadcasted_iota(jnp.int32, (length, length), 1)
    ).astype(F32).astype(BF16)
    high, middle, low = in_three(rates)
    climb = dot(low, upper) + dot(middle, upper) + dot(high, upper)
    end = climb[:, length - 1 :]
    spot = lax.broadcasted_iota(jnp.int32, (heads, length), 1)
    tail = jnp.where(spot >= last_start - offset, jnp.exp(climb - end) * steps, 0.0)
    entry = jnp.where(spot < first_here - offset, jnp.exp(-climb), 0.0)
    rs[...] = jnp.zeros(rs.shape, F32)
    rs[0:heads] = climb
    rs[16 : 16 + heads] = tail
    rs[32 : 32 + heads] = entry
    cols = rs[...].T
    cols_ref[...] = cols
    rows_ref[...] = jnp.zeros(rows_ref.shape, F32)
    rows_ref[0:heads] = climb
    rows_ref[16 : 16 + heads] = steps
    keys = kq_ref[:, :STATE].astype(F32).T.astype(BF16)
    for j in range(width // LANES):
        sl = slice(j * LANES, (j + 1) * LANES)
        value = conv(xs, cw_ref, cb_ref, j * LANES)
        val_ref[:, sl] = value
        high, low = in_two(value.astype(F32) * pair_of(cols, 16 + 2 * j))
        e_ref[:, sl] = dot(keys, high) + dot(keys, low)
        d_ref[:, sl] = pair_of(cols[length - 8 :], 32 + 2 * j)


def intra_kernel(lens, offset_ref, kq_ref, val_ref, cols_ref, rows_ref, y_ref):
    length, width = val_ref.shape
    offset = offset_ref[0]
    _, found = own_starts(lens, offset, length)
    found = found - offset
    lane = lax.broadcasted_iota(jnp.int32, (LANES, LANES), 1)
    for i in range(length // LANES):
        rows = slice(i * LANES, (i + 1) * LANES)
        upto = (i + 1) * LANES
        scores = dot(kq_ref[rows, STATE:], kq_ref[:upto, :STATE], 1, 1)
        t = i * LANES + lax.broadcasted_iota(jnp.int32, (LANES, upto), 0)
        s = lax.broadcasted_iota(jnp.int32, (LANES, upto), 1)
        scores = jnp.where((s <= t) & (s >= found[rows, 0:1]), scores, 0.0)
        for j in range(width // LANES):
            sl = slice(j * LANES, (j + 1) * LANES)
            both = []
            for h in (2 * j, 2 * j + 1):
                gap = rows_ref[h : h + 1, :upto] - cols_ref[rows, h : h + 1]
                weight = jnp.exp(jnp.minimum(gap, 0.0)) * scores * rows_ref[16 + h : 17 + h, :upto]
                high, low = in_two(weight)
                both.append(dot(high, val_ref[:upto, sl]) + dot(low, val_ref[:upto, sl]))
            y_ref[rows, sl] = jnp.where(lane < HEAD_SIZE, both[0], both[1])


def gate_kernel(kq_ref, s_ref, cols_ref, y_ref, val_ref, z_ref, skip_ref, g_ref, ss_ref):
    length, width = val_ref.shape
    cols = cols_ref[...]
    total = jnp.zeros((length, LANES), F32)
    for j in range(width // LANES):
        sl = slice(j * LANES, (j + 1) * LANES)
        high, low = in_two(s_ref[:, sl])
        far = dot(kq_ref[:, STATE:], high) + dot(kq_ref[:, STATE:], low)
        out = y_ref[:, sl] + far * pair_of(cols, 32 + 2 * j)
        mixed = out + skip_ref[:, sl] * val_ref[:, sl].astype(F32)
        gated = mixed * silu(z_ref[:, sl].astype(F32))
        g_ref[:, sl] = gated
        total = total + gated * gated
    ss_ref[...] = jnp.sum(total.T, axis=0, keepdims=True)


def project_first_kernel(order, w_ref, p0, p1, p2, p3, p4, p5, acc_ref):
    total = jnp.zeros(acc_ref.shape, F32)
    for k, piece in enumerate((p0, p1, p2, p3, p4, p5)):
        total = total + dot(w_ref[order[k]], piece[...], 1, 1)
    acc_ref[...] = total


def project_last_kernel(order, w_ref, acc_ref, res_ref, a0, b0, a1, b1, out_ref):
    half = a0.shape[0]
    for at, pieces in ((0, (a0, a1)), (half, (b0, b1))):
        sl = slice(at, at + half)
        total = acc_ref[:, sl]
        for k, piece in enumerate(pieces):
            total = total + dot(w_ref[order[6 + k]], piece[...], 1, 1)
        out_ref[:, sl] = (res_ref[:, sl].astype(F32) + total).astype(BF16)


def logits_kernel(order, meta, *refs, members, overlap):
    per = 10
    pieces = [refs[m * per : (m + 1) * per] for m in range(members)]
    gain_ref, target_ref, w_ref, out_ref, wide, hid, peak, total, pick, want = refs[members * per :]
    step = pl.program_id(0)
    block = w_ref.shape[1]
    depth = wide.shape[0]
    length = wide.shape[1]
    rows = members * length

    @pl.when(step == 0)
    def _():
        for m in range(members):
            part = pieces[m][0].shape[0]
            squares = jnp.zeros((1, length), F32)
            for k in range(6):
                piece = pieces[m][k][...]
                at = pl.multiple_of(order[k] * part, 64)
                wide[pl.ds(at, part), :] = piece
                big = piece.astype(F32)
                squares = squares + jnp.sum(big * big, axis=0, keepdims=True)
            for k in range(2):
                at = pl.multiple_of(order[6 + k] * part, 64)
                piece = jnp.concatenate([pieces[m][6 + 2 * k][...], pieces[m][7 + 2 * k][...]], axis=1)
                wide[pl.ds(at, part), :] = piece
                big = piece.astype(F32)
                squares = squares + jnp.sum(big * big, axis=0, keepdims=True)
            scale = lax.rsqrt(squares / depth + EPSILON)
            for at in range(0, depth, LANES):
                sl = slice(at, at + LANES)
                value = wide[sl, :].astype(F32) * scale * gain_ref[sl, :]
                hid[m * length : (m + 1) * length, sl] = value.T.astype(BF16)
        want[...] = jnp.zeros((rows, LANES), jnp.int32) + target_ref[...]
        peak[...] = jnp.full((rows, LANES), NEG, F32)
        total[...] = jnp.zeros((rows, LANES), F32)
        pick[...] = jnp.zeros((rows, LANES), F32)

    chunk = 256
    for r in range(0, rows, chunk):
        rw = slice(r, r + chunk)
        logits = dot(hid[rw, :], w_ref[...])
        lane = lax.broadcasted_iota(jnp.int32, (chunk, LANES), 1)
        groups = []
        found = pick[rw, :]
        old = peak[rw, :]
        top = old
        for g in range(block // LANES):
            at = step * block + g * LANES
            part = logits[:, g * LANES : (g + 1) * LANES]
            good = (meta[0] == 0) | (at >= overlap)
            part = jnp.where(good, part, NEG)
            groups.append(part)
            found = found + jnp.where((lane + (at + meta[1]) == want[rw, :]) & good, part, 0.0)
            top = jnp.maximum(top, part)
        add = total[rw, :] * jnp.exp(old - top)
        for part in groups:
            add = add + jnp.exp(part - top)
        pick[rw, :] = found
        peak[rw, :] = top
        total[rw, :] = add

    @pl.when(step == pl.num_programs(0) - 1)
    def _():
        tops = peak[...].T
        top = jnp.max(tops, axis=0, keepdims=True)
        out_ref[0:1, :] = top + jnp.log(jnp.sum(total[...].T * jnp.exp(tops - top), axis=0, keepdims=True))
        out_ref[1:2, :] = jnp.sum(pick[...].T, axis=0, keepdims=True)


def shape(dims, dtype):
    return jax.ShapeDtypeStruct(dims, dtype)


def cost(flops, nbytes):
    return pl.CostEstimate(flops=int(flops), bytes_accessed=int(nbytes), transcendentals=0)


def ring(length, by):
    return [(i, (i + by) % length) for i in range(length)]


def swapped(length, bit):
    return [(i, i ^ bit) for i in range(length)]


def around_x(piece, dim):
    size = lax.axis_size("x")
    half = piece.shape[dim] // 2
    left = lax.ppermute(piece, "x", ring(size, 1))
    right = lax.ppermute(piece, "x", ring(size, -1))
    own_other = lax.ppermute(piece, "core", swapped(2, 1))
    far_a = lax.ppermute(lax.slice_in_dim(left, 0, half, axis=dim), "x", ring(size, 1))
    far_b = lax.ppermute(lax.slice_in_dim(right, half, 2 * half, axis=dim), "x", ring(size, -1))
    left_other = lax.ppermute(left, "core", swapped(2, 1))
    right_other = lax.ppermute(right, "core", swapped(2, 1))
    far_a_other = lax.ppermute(far_a, "core", swapped(2, 1))
    far_b_other = lax.ppermute(far_b, "core", swapped(2, 1))
    near = (piece, own_other, left, left_other, right, right_other)
    return near, (far_a, far_b, far_a_other, far_b_other)


def order_here():
    size = lax.axis_size("x")
    x, core = lax.axis_index("x"), lax.axis_index("core")
    spots = [x, x, x - 1, x - 1, x + 1, x + 1, x + 2, x + 2]
    return jnp.stack(
        [2 * lax.rem(s + size, size) + (1 - core if k % 2 else core) for k, s in enumerate(spots)]
    ).astype(jnp.int32)


def lse_of(parts):
    top = functools.reduce(jnp.maximum, [p[0:1] for p in parts])
    total = sum(jnp.exp(p[0:1] - top) for p in parts)
    return jnp.concatenate([top + jnp.log(total), sum(p[1:2] for p in parts)], axis=0)


def local(
    residual, x_in, bc_in, z_in, dt_raw, dt_bias, decay_rate, d_skip, conv_x_weight, conv_x_bias,
    conv_bc_weight, conv_bc_bias, norm_gain, out_weight, final_gain, lm_weight, targets, doc_lengths,
):
    length, inner = x_in.shape
    heads = dt_raw.shape[0]
    ranks = lax.axis_size(HEADS_AXES)
    seq_size = lax.axis_size("seq")
    groups = lax.axis_size("groups")
    seq_rank = lax.axis_index("seq")
    head_rank = lax.axis_index(HEADS_AXES)
    parity = lax.rem(lax.axis_index("groups"), 2)
    mates = swapped(groups, 1)
    offset = (seq_rank * length).reshape(1).astype(jnp.int32)
    share = residual.shape[1]
    depth = share * ranks

    vocab = lm_weight.shape[1]
    block = 256
    width = -(-vocab // (2 * block)) * block
    overlap = 2 * width - vocab
    first_column = parity * (vocab - width)
    mine = lax.dynamic_slice_in_dim(lm_weight, first_column, width, 1)
    embedding = lax.all_gather(mine, "seq", axis=0, tiled=True)

    onward = [(i, i + 1) for i in range(seq_size - 1)]
    x_rim, bc_rim = lax.ppermute((x_in[length - RIM :], bc_in[length - RIM :]), "seq", onward)
    head_table = jnp.stack([dt_bias, decay_rate], axis=1)
    values, kq, cols, rows, state, through = pl.pallas_call(
        front_kernel,
        out_shape=(
            shape((length, inner), BF16),
            shape((length, 2 * STATE), BF16),
            shape((length, LANES), F32),
            shape((32, length), F32),
            shape((STATE, inner), F32),
            shape((8, inner), F32),
        ),
        in_specs=[SMEM, SMEM] + [pl.BlockSpec()] * 10,
        scratch_shapes=[
            pltpu.VMEM((length + RIM, inner), F32),
            pltpu.VMEM((length + RIM, 2 * STATE), F32),
            pltpu.VMEM((LANES, length), F32),
        ],
        name="front",
    )(
        doc_lengths, offset, x_in, x_rim, bc_in, bc_rim, dt_raw, head_table,
        conv_x_weight, conv_x_bias[None], conv_bc_weight, conv_bc_bias[None],
    )

    incoming = lax.ppermute(state, "seq", onward)
    for _ in range(-(-(LONGEST - 1) // length) - 1):
        incoming = lax.ppermute(state + through[7:8] * incoming, "seq", onward)

    inside = pl.pallas_call(
        intra_kernel,
        out_shape=shape((length, inner), F32),
        in_specs=[SMEM, SMEM] + [pl.BlockSpec()] * 4,
        cost_estimate=cost(16e9, 4e6),
        name="intra",
    )(doc_lengths, offset, kq, values, cols, rows)

    out_weight, _ = lax.optimization_barrier((out_weight, through))
    turned = out_weight.T.reshape(ranks, share, inner)
    weights = lax.all_to_all(turned, HEADS_AXES, 0, 0, tiled=True)

    skip = jnp.repeat(d_skip, HEAD_SIZE)[None]
    gated, squares = pl.pallas_call(
        gate_kernel,
        out_shape=(shape((length, inner), F32), shape((1, length), F32)),
        name="gate",
    )(kq, incoming, cols, inside, values, z_in, skip)
    squares = lax.psum(squares, HEADS_AXES)
    scale = lax.rsqrt(squares[0] / (inner * ranks) + EPSILON)
    normed = (gated * scale[:, None] * norm_gain.astype(F32)[None, :]).astype(BF16)

    order = order_here()
    near, far = around_x(normed, 0)
    partial = pl.pallas_call(
        project_first_kernel,
        out_shape=shape((share, length), F32),
        in_specs=[SMEM] + [pl.BlockSpec()] * 7,
        cost_estimate=cost(6e9, 8e6),
        name="project_first",
    )(order, weights, *near)
    far_a, far_b, far_a_other, far_b_other = far
    block_out = pl.pallas_call(
        project_last_kernel,
        out_shape=shape((share, length), BF16),
        in_specs=[SMEM] + [pl.BlockSpec()] * 7,
        name="project_last",
    )(order, weights, partial, residual.T, far_a, far_b, far_a_other, far_b_other)

    theirs = lax.ppermute(block_out, "groups", mates)
    near, far = around_x(block_out, 1)
    their_near, their_far = around_x(theirs, 1)
    their_targets = lax.ppermute(targets, "groups", mates)
    wanted = jnp.concatenate([targets, their_targets]) - head_rank * vocab
    meta = jnp.stack([parity, first_column]).astype(jnp.int32)
    members = 2
    whole = pl.BlockSpec()
    losses = pl.pallas_call(
        functools.partial(logits_kernel, members=members, overlap=overlap),
        out_shape=shape((2, members * length), F32),
        grid=(width // block,),
        in_specs=[SMEM, SMEM] + [whole] * 22 + [pl.BlockSpec((depth, block), lambda i: (0, i))],
        out_specs=pl.BlockSpec((2, members * length), lambda i: (0, 0)),
        scratch_shapes=[
            pltpu.VMEM((depth, length), BF16),
            pltpu.VMEM((members * length, depth), BF16),
            pltpu.VMEM((members * length, LANES), F32),
            pltpu.VMEM((members * length, LANES), F32),
            pltpu.VMEM((members * length, LANES), F32),
            pltpu.VMEM((members * length, LANES), jnp.int32),
        ],
        name="logits",
    )(
        order, meta, *near, *far, *their_near, *their_far,
        final_gain.astype(F32)[:, None], wanted[:, None], embedding,
    )

    given = lax.ppermute(losses[:, length:], "groups", mates)
    parts = lse_of([losses[:, :length], given])
    parts = lse_of([parts, lax.ppermute(parts, "core", swapped(2, 1))])
    size = lax.axis_size("x")
    parts = lse_of([parts] + [lax.ppermute(parts, "x", ring(size, k)) for k in range(1, size)])
    tokens = (parts[0:1] - parts[1:2])[0]

    ends = jnp.cumsum(doc_lengths)
    positions = offset[0] + jnp.arange(length, dtype=jnp.int32)
    member = (positions[:, None] < ends[None, :]) & (positions[:, None] >= (ends - doc_lengths)[None, :])
    sums = jnp.sum(jnp.where(member, tokens[:, None], 0.0), axis=0)
    everyone = jnp.broadcast_to(sums[None, None], (seq_size, 1, sums.shape[0]))
    sums = lax.all_to_all(everyone, "seq", 0, 0, tiled=True).sum(axis=(0, 1))
    return block_out.T, sums / doc_lengths.astype(F32)


def solution(mesh):
    groups, seq, head = (mesh.shape[name] for name in ("groups", "seq", "head"))
    split = Mesh(mesh.devices.reshape(groups, seq, head // 2, 2), ("groups", "seq", "x", "core"))
    tokens = ("groups", "seq")
    heads = HEADS_AXES
    in_specs = (
        P(tokens, heads), P(tokens, heads), P(tokens, None), P(tokens, heads), P(heads, tokens),
        P(heads), P(heads), P(heads), P(None, heads), P(heads), P(), P(), P(heads), P(heads, None),
        P(), P("seq", heads), P(tokens), P("groups"),
    )
    out_specs = (P(tokens, heads), P("groups"))
    return jax.shard_map(local, mesh=split, in_specs=in_specs, out_specs=out_specs, check_vma=False)
```

```python
import functools

import jax
import jax.numpy as jnp
from jax import lax
from jax.experimental import pallas as pl
from jax.experimental.pallas import tpu as pltpu
from jax.sharding import Mesh
from jax.sharding import PartitionSpec as P


STATE = 128
HEAD_SIZE = 64
KERNEL = 4
LONGEST = 1536
EPSILON = 1e-05
LANES = 128
RIM = 8
NEG = -1e30
F32 = jnp.float32
BF16 = jnp.bfloat16

SMEM = pl.BlockSpec(memory_space=pltpu.SMEM)
HEADS_AXES = ("x", "core")


def dot(a, b, ca=1, cb=0):
    return lax.dot_general(a, b, (((ca,), (cb,)), ((), ())), preferred_element_type=F32)


def in_two(value):
    high = value.astype(BF16)
    return high, (value - high.astype(F32)).astype(BF16)


def in_three(value):
    high = value.astype(BF16)
    rest = value - high.astype(F32)
    middle = rest.astype(BF16)
    return high, middle, (rest - middle.astype(F32)).astype(BF16)


def silu(value):
    return value * jax.nn.sigmoid(value)


def starts_of(lens):
    start = jnp.int32(0)
    for d in range(lens.shape[0]):
        yield start
        start = start + lens[d]


def own_starts(lens, offset, length):
    pos = offset + lax.broadcasted_iota(jnp.int32, (length, LANES), 0)
    found = jnp.zeros((length, LANES), jnp.int32)
    for start in starts_of(lens):
        found = jnp.where(pos >= start, start, found)
    return pos, found


def pair_of(cols, at):
    lane = lax.broadcasted_iota(jnp.int32, (cols.shape[0], LANES), 1)
    return jnp.where(lane < HEAD_SIZE, cols[:, at : at + 1], cols[:, at + 1 : at + 2])


def front_kernel(
    lens, offset_ref, x_ref, bc_ref, rim_ref, dt_ref, hp_ref, cw_ref, cb_ref, bw_ref, bb_ref,
    val_ref, kq_ref, cols_ref, rows_ref, e_ref, d_ref, xs, bs, rs,
):
    length, width = x_ref.shape
    heads = dt_ref.shape[0]
    offset = offset_ref[0]
    pos, found = own_starts(lens, offset, length)
    depth = pos - found
    last_start = jnp.int32(0)
    first_here = jnp.int32(2**30)
    for start in starts_of(lens):
        last_start = jnp.where(start <= offset + length - 1, start, last_start)
        first_here = jnp.where(start >= offset, jnp.minimum(first_here, start), first_here)

    bs[:RIM] = rim_ref[:, width:].astype(F32)
    bs[RIM:] = bc_ref[...].astype(F32)
    xs[:RIM] = rim_ref[:, :width].astype(F32)
    xs[RIM:] = x_ref[...].astype(F32)

    def conv(buf, w_ref, b_ref, at):
        sl = slice(at, at + LANES)
        total = jnp.zeros((length, LANES), F32) + b_ref[:, sl].astype(F32)
        for k in range(KERNEL):
            lag = KERNEL - 1 - k
            tap = w_ref[k : k + 1, sl].astype(F32) * buf[RIM - lag : RIM - lag + length, sl]
            total = total + (jnp.where(depth >= lag, tap, 0.0) if lag else tap)
        return silu(total).astype(BF16)

    for at in range(0, 2 * STATE, LANES):
        kq_ref[:, at : at + LANES] = conv(bs, bw_ref, bb_ref, at)

    hp = hp_ref[...]
    raw = dt_ref[...] + hp[:, 0:1]
    steps = jnp.maximum(raw, 0.0) + jnp.log1p(jnp.exp(-jnp.abs(raw)))
    rates = steps * hp[:, 1:2]
    upper = (
        lax.broadcasted_iota(jnp.int32, (length, length), 0)
        <= lax.broadcasted_iota(jnp.int32, (length, length), 1)
    ).astype(F32).astype(BF16)
    high, middle, low = in_three(rates)
    climb = dot(low, upper) + dot(middle, upper) + dot(high, upper)
    end = climb[:, length - 1 :]
    spot = lax.broadcasted_iota(jnp.int32, (heads, length), 1)
    tail = jnp.where(spot >= last_start - offset, jnp.exp(climb - end) * steps, 0.0)
    entry = jnp.where(spot < first_here - offset, jnp.exp(-climb), 0.0)
    rs[...] = jnp.zeros(rs.shape, F32)
    rs[0:heads] = climb
    rs[16 : 16 + heads] = tail
    rs[32 : 32 + heads] = entry
    cols = rs[...].T
    cols_ref[...] = cols
    rows_ref[...] = jnp.zeros(rows_ref.shape, F32)
    rows_ref[0:heads] = climb
    rows_ref[16 : 16 + heads] = steps
    keys = kq_ref[:, :STATE].astype(F32).T.astype(BF16)
    for j in range(width // LANES):
        sl = slice(j * LANES, (j + 1) * LANES)
        value = conv(xs, cw_ref, cb_ref, j * LANES)
        val_ref[:, sl] = value
        high, low = in_two(value.astype(F32) * pair_of(cols, 16 + 2 * j))
        e_ref[:, sl] = dot(keys, high) + dot(keys, low)
        d_ref[:, sl] = pair_of(cols[length - 8 :], 32 + 2 * j)


def intra_kernel(lens, offset_ref, kq_ref, val_ref, cols_ref, rows_ref, y_ref):
    length, width = val_ref.shape
    offset = offset_ref[0]
    _, found = own_starts(lens, offset, length)
    found = found - offset
    lane = lax.broadcasted_iota(jnp.int32, (LANES, LANES), 1)
    for i in range(length // LANES):
        rows = slice(i * LANES, (i + 1) * LANES)
        upto = (i + 1) * LANES
        scores = dot(kq_ref[rows, STATE:], kq_ref[:upto, :STATE], 1, 1)
        t = i * LANES + lax.broadcasted_iota(jnp.int32, (LANES, upto), 0)
        s = lax.broadcasted_iota(jnp.int32, (LANES, upto), 1)
        scores = jnp.where((s <= t) & (s >= found[rows, 0:1]), scores, 0.0)
        for j in range(width // LANES):
            sl = slice(j * LANES, (j + 1) * LANES)
            both = []
            for h in (2 * j, 2 * j + 1):
                gap = rows_ref[h : h + 1, :upto] - cols_ref[rows, h : h + 1]
                weight = jnp.exp(jnp.minimum(gap, 0.0)) * scores * rows_ref[16 + h : 17 + h, :upto]
                high, low = in_two(weight)
                both.append(dot(high, val_ref[:upto, sl]) + dot(low, val_ref[:upto, sl]))
            y_ref[rows, sl] = jnp.where(lane < HEAD_SIZE, both[0], both[1])


def gate_kernel(kq_ref, s_ref, cols_ref, y_ref, val_ref, z_ref, skip_ref, g_ref, ss_ref):
    length, width = val_ref.shape
    cols = cols_ref[...]
    total = jnp.zeros((length, LANES), F32)
    for j in range(width // LANES):
        sl = slice(j * LANES, (j + 1) * LANES)
        high, low = in_two(s_ref[:, sl])
        far = dot(kq_ref[:, STATE:], high) + dot(kq_ref[:, STATE:], low)
        out = y_ref[:, sl] + far * pair_of(cols, 32 + 2 * j)
        mixed = out + skip_ref[:, sl] * val_ref[:, sl].astype(F32)
        gated = mixed * silu(z_ref[:, sl].astype(F32))
        g_ref[:, sl] = gated
        total = total + gated * gated
    ss_ref[...] = jnp.sum(total.T, axis=0, keepdims=True)


def project_kernel(*refs, count):
    pieces, weights, acc_ref, out_ref = refs[:count], refs[count : 2 * count], refs[2 * count], refs[-1]
    total = None
    for piece, weight in zip(pieces, weights):
        part = dot(weight[...], piece[...], 1, 1)
        total = part if total is None else total + part
    out_ref[...] = total if acc_ref is out_ref else acc_ref[...] + total


def project_last_kernel(w0, w1, acc_ref, res_ref, a0, b0, a1, b1, out_ref):
    half = a0.shape[0]
    for at, pieces in ((0, (a0, a1)), (half, (b0, b1))):
        sl = slice(at, at + half)
        total = acc_ref[:, sl]
        for weight, piece in zip((w0, w1), pieces):
            total = total + dot(weight[...], piece[...], 1, 1)
        out_ref[:, sl] = (res_ref[:, sl].astype(F32) + total).astype(BF16)


def logits_kernel(
    meta, *refs, overlap, width,
):
    pieces = refs[:16]
    gain_ref, target_ref, w_ref, out_ref, wide, hid, peak, total, pick, want, lg = refs[16:]
    step = pl.program_id(0)
    block = w_ref.shape[1]
    depth = wide.shape[0]
    part, length = pieces[0].shape
    members = 2
    rows = members * length

    @pl.when(step == 0)
    def _():
        for m in range(members):
            squares = jnp.zeros((1, length), F32)
            for k in range(8):
                piece = pieces[4 * (k // 2) + 2 * m + k % 2][...]
                chip = (meta[2] + (0, 3, 1, 2)[k // 2]) % 4
                rank = 2 * chip + (1 - meta[3] if k % 2 else meta[3])
                wide[pl.ds(pl.multiple_of(rank * part, 64), part), :] = piece
                big = piece.astype(F32)
                squares = squares + jnp.sum(big * big, axis=0, keepdims=True)
            scale = lax.rsqrt(squares / depth + EPSILON)
            for at in range(0, depth, LANES):
                sl = slice(at, at + LANES)
                value = (wide[sl, :].astype(F32) * scale).T * gain_ref[:, sl].astype(F32)
                hid[m * length : (m + 1) * length, sl] = value.astype(BF16)
        want[...] = jnp.zeros((rows, LANES), jnp.int32) + target_ref[...]
        peak[...] = jnp.full((rows, LANES), NEG, F32)
        total[...] = jnp.zeros((rows, LANES), F32)
        pick[...] = jnp.zeros((rows, LANES), F32)

    lg[...] = dot(hid[...], w_ref[...])
    chunk = 128

    def fold(i, _):
        rw = pl.ds(pl.multiple_of(i * chunk, chunk), chunk)
        lane = lax.broadcasted_iota(jnp.int32, (chunk, LANES), 1)
        found = pick[rw, :]
        old = peak[rw, :]
        top = old
        groups = []
        for g in range(block // LANES):
            at = step * block + g * LANES
            good = ((meta[0] == 0) | (at >= overlap)) & (at < width)
            part = jnp.where(good, lg[rw, g * LANES : (g + 1) * LANES], NEG)
            groups.append(part)
            found = found + jnp.where((lane + (at + meta[1]) == want[rw, :]) & good, part, 0.0)
            top = jnp.maximum(top, part)
        add = total[rw, :] * jnp.exp(old - top)
        for part in groups:
            add = add + jnp.exp(part - top)
        pick[rw, :] = found
        peak[rw, :] = top
        total[rw, :] = add
        return 0

    lax.fori_loop(0, rows // chunk, fold, 0)

    @pl.when(step == pl.num_programs(0) - 1)
    def _():
        tops = peak[...].T
        top = jnp.max(tops, axis=0, keepdims=True)
        out_ref[0:1, :] = top + jnp.log(jnp.sum(total[...].T * jnp.exp(tops - top), axis=0, keepdims=True))
        out_ref[1:2, :] = jnp.sum(pick[...].T, axis=0, keepdims=True)


def shape(dims, dtype):
    return jax.ShapeDtypeStruct(dims, dtype)


def cost(flops, nbytes):
    return pl.CostEstimate(flops=int(flops), bytes_accessed=int(nbytes), transcendentals=0)


def ring(length, by):
    return [(i, (i + by) % length) for i in range(length)]


def swapped(length, bit):
    return [(i, i ^ bit) for i in range(length)]


def from_chips(value, by):
    return lax.ppermute(value, "x", ring(lax.axis_size("x"), by))


def from_core(value):
    return lax.ppermute(value, "core", swapped(2, 1))


def summed_over_heads(value):
    value = value + from_core(value)
    return value + sum(from_chips(value, k) for k in range(1, lax.axis_size("x")))


def order_here():
    size = lax.axis_size("x")
    x, core = lax.axis_index("x"), lax.axis_index("core")
    spots = [x, x, x - 1, x - 1, x + 1, x + 1, x + 2, x + 2]
    return jnp.stack(
        [2 * lax.rem(s + size, size) + (1 - core if k % 2 else core) for k, s in enumerate(spots)]
    ).astype(jnp.int32)


def lse_of(parts):
    top = functools.reduce(jnp.maximum, [p[0:1] for p in parts])
    total = sum(jnp.exp(p[0:1] - top) for p in parts)
    return jnp.concatenate([top + jnp.log(total), sum(p[1:2] for p in parts)], axis=0)


def compute(
    residual, x_in, bc_in, z_in, dt_raw, dt_bias, decay_rate, d_skip, conv_x_weight, conv_x_bias,
    conv_bc_weight, conv_bc_bias, norm_gain, out_weight, final_gain, lm_weight, targets, doc_lengths,
):
    length, inner = x_in.shape
    ranks = lax.axis_size(HEADS_AXES)
    seq_size = lax.axis_size("seq")
    groups = lax.axis_size("groups")
    seq_rank = lax.axis_index("seq")
    head_rank = lax.axis_index(HEADS_AXES)
    parity = lax.rem(lax.axis_index("groups"), 2)
    mates = swapped(groups, 1)
    offset = (seq_rank * length).reshape(1).astype(jnp.int32)
    share = residual.shape[1]
    depth = share * ranks

    onward = [(i, i + 1) for i in range(seq_size - 1)]
    rim = jnp.concatenate([x_in[length - RIM :], bc_in[length - RIM :]], axis=1)
    rim = lax.ppermute(rim, "seq", onward)

    head_table = jnp.stack([dt_bias, decay_rate], axis=1)
    values, kq, cols, rows, state, through = pl.pallas_call(
        front_kernel,
        out_shape=(
            shape((length, inner), BF16),
            shape((length, 2 * STATE), BF16),
            shape((length, LANES), F32),
            shape((32, length), F32),
            shape((STATE, inner), F32),
            shape((8, inner), F32),
        ),
        in_specs=[SMEM, SMEM] + [pl.BlockSpec()] * 9,
        scratch_shapes=[
            pltpu.VMEM((length + RIM, inner), F32),
            pltpu.VMEM((length + RIM, 2 * STATE), F32),
            pltpu.VMEM((LANES, length), F32),
        ],
        name="front",
    )(
        doc_lengths, offset, x_in, bc_in, rim, dt_raw, head_table,
        conv_x_weight, conv_x_bias[None], conv_bc_weight, conv_bc_bias[None],
    )

    incoming = lax.ppermute(state, "seq", onward)
    through, out_weight, targets, d_skip = lax.optimization_barrier((through, out_weight, targets, d_skip))
    incoming, lm_weight = lax.optimization_barrier((incoming, lm_weight))
    for _ in range(2, -(-(LONGEST - 1) // length) + 1):
        carried = state + through[7:8] * incoming
        incoming = lax.ppermute(carried, "seq", onward)

    vocab = lm_weight.shape[1]
    block = 256
    width = -(-vocab // (2 * LANES)) * LANES
    overlap = 2 * width - vocab
    first_column = parity * (vocab - width)
    mine = lax.dynamic_slice_in_dim(lm_weight, first_column, width, 1)
    embedding = lax.all_gather(mine, "seq", axis=0, tiled=True)

    order = order_here()
    meta = jnp.stack([parity, first_column, lax.axis_index("x"), lax.axis_index("core")]).astype(jnp.int32)
    their_targets = lax.ppermute(targets, "groups", mates)
    wanted = (jnp.concatenate([targets, their_targets]) - head_rank * vocab)[:, None]
    skip = jnp.repeat(d_skip, HEAD_SIZE)[None]
    turned = out_weight.T.reshape(ranks, share, inner)
    weights = lax.all_to_all(turned, HEADS_AXES, 0, 0, tiled=True)

    inside = pl.pallas_call(
        intra_kernel,
        out_shape=shape((length, inner), F32),
        in_specs=[SMEM, SMEM] + [pl.BlockSpec()] * 4,
        cost_estimate=cost(5e9, 4e6),
        name="intra",
    )(doc_lengths, offset, kq, values, cols, rows)
    by_rank = [lax.dynamic_index_in_dim(weights, order[k], 0, False) for k in range(ranks)]
    incoming, meta, wanted, skip = lax.optimization_barrier((incoming, meta, wanted, skip))

    gated, squares = pl.pallas_call(
        gate_kernel,
        out_shape=(shape((length, inner), F32), shape((1, length), F32)),
        name="gate",
    )(kq, incoming, cols, inside, values, z_in, skip)
    squares = summed_over_heads(squares)
    scale = lax.rsqrt(squares[0] / (inner * ranks) + EPSILON)
    normed = (gated * scale[:, None] * norm_gain.astype(F32)[None, :]).astype(BF16)

    left = from_chips(normed, 1)
    right = from_chips(normed, -1)
    other = from_core(normed)
    half = length // 2
    projected = pl.pallas_call(
        functools.partial(project_kernel, count=2),
        out_shape=shape((share, length), F32),
        cost_estimate=cost(3e9, 4e6),
        name="project_own",
    )(normed, other, *by_rank[:2])
    left, right, projected = lax.optimization_barrier((left, right, projected))
    far_a = from_chips(left[:half], 1)
    far_b = from_chips(right[half:], -1)
    left_other = from_core(left)
    right_other = from_core(right)
    projected = pl.pallas_call(
        functools.partial(project_kernel, count=4),
        out_shape=shape((share, length), F32),
        cost_estimate=cost(3e9, 4e6),
        name="project_near",
    )(left, left_other, right, right_other, *by_rank[2:6], projected)
    far_a, far_b, projected = lax.optimization_barrier((far_a, far_b, projected))
    block_out = pl.pallas_call(
        project_last_kernel,
        out_shape=shape((share, length), BF16),
        name="project_far",
    )(*by_rank[6:8], projected, residual.T, far_a, far_b, from_core(far_a), from_core(far_b))

    own1 = lax.ppermute(block_out, "groups", mates)
    own0 = block_out
    left0, right0 = from_chips(own0, 1), from_chips(own0, -1)
    left1, right1 = from_chips(own1, 1), from_chips(own1, -1)
    far0 = from_chips(left0, 1)
    far1 = from_chips(right1, -1)
    mine = (own0, own1, left0, left1, right0, right1, far0, far1)
    pieces = [p for own in mine for p in (own, from_core(own))]
    whole = pl.BlockSpec()
    losses = pl.pallas_call(
        functools.partial(logits_kernel, overlap=overlap, width=width),
        out_shape=shape((2, 2 * length), F32),
        grid=(-(-width // block),),
        in_specs=[SMEM] + [whole] * 18 + [pl.BlockSpec((depth, block), lambda i: (0, i))],
        out_specs=pl.BlockSpec((2, 2 * length), lambda i: (0, 0)),
        scratch_shapes=[
            pltpu.VMEM((depth, length), BF16),
            pltpu.VMEM((2 * length, depth), BF16),
            pltpu.VMEM((2 * length, LANES), F32),
            pltpu.VMEM((2 * length, LANES), F32),
            pltpu.VMEM((2 * length, LANES), F32),
            pltpu.VMEM((2 * length, LANES), jnp.int32),
            pltpu.VMEM((2 * length, block), F32),
        ],
        name="logits",
    )(
        meta, *pieces, final_gain[None], wanted, embedding,
    )

    mine, given = losses[:, :length], losses[:, length:]
    axes = ("groups", "core")
    across = [(2 * g + c, 2 * (g ^ 1) + (c ^ 1)) for g in range(groups) for c in range(2)]
    parts = lse_of(
        [mine, from_core(mine), lax.ppermute(given, "groups", mates), lax.ppermute(given, axes, across)]
    )
    parts = lse_of([parts] + [from_chips(parts, k) for k in range(1, lax.axis_size("x"))])
    tokens = (parts[0:1] - parts[1:2])[0]

    ends = jnp.cumsum(doc_lengths)
    positions = offset[0] + jnp.arange(length, dtype=jnp.int32)
    member = (positions[:, None] < ends[None, :]) & (positions[:, None] >= (ends - doc_lengths)[None, :])
    sums = jnp.sum(jnp.where(member, tokens[:, None], 0.0), axis=0)
    everyone = jnp.broadcast_to(sums[None, None], (seq_size, 1, sums.shape[0]))
    sums = lax.all_to_all(everyone, "seq", 0, 0, tiled=True).sum(axis=(0, 1))
    return block_out.T, sums / doc_lengths.astype(F32)


def solution(mesh):
    groups, seq, head = (mesh.shape[name] for name in ("groups", "seq", "head"))
    split = Mesh(mesh.devices.reshape(groups, seq, head // 2, 2), ("groups", "seq", "x", "core"))
    tokens = ("groups", "seq")
    heads = HEADS_AXES
    in_specs = (
        P(tokens, heads), P(tokens, heads), P(tokens, None), P(tokens, heads), P(heads, tokens),
        P(heads), P(heads), P(heads), P(None, heads), P(heads), P(), P(), P(heads), P(heads, None),
        P(), P("seq", heads), P(tokens), P("groups"),
    )
    out_specs = (P(tokens, heads), P("groups"))
    return jax.shard_map(compute, mesh=split, in_specs=in_specs, out_specs=out_specs, check_vma=False)
```

```python
import functools

import jax
import jax.numpy as jnp
from jax import lax
from jax.experimental import pallas as pl
from jax.experimental.pallas import tpu as pltpu
from jax.sharding import Mesh
from jax.sharding import PartitionSpec as P


STATE = 128
HEAD_SIZE = 64
KERNEL = 4
LONGEST = 1536
EPSILON = 1e-05
LANES = 128
RIM = 8
NEG = -1e30
F32 = jnp.float32
BF16 = jnp.bfloat16

SMEM = pl.BlockSpec(memory_space=pltpu.SMEM)
HEADS_AXES = ("x", "core")


def dot(a, b, ca=1, cb=0):
    return lax.dot_general(a, b, (((ca,), (cb,)), ((), ())), preferred_element_type=F32)


def in_two(value):
    high = value.astype(BF16)
    return high, (value - high.astype(F32)).astype(BF16)


def in_three(value):
    high = value.astype(BF16)
    rest = value - high.astype(F32)
    middle = rest.astype(BF16)
    return high, middle, (rest - middle.astype(F32)).astype(BF16)


def silu(value):
    return value * jax.nn.sigmoid(value)


def starts_of(lens):
    start = jnp.int32(0)
    for d in range(lens.shape[0]):
        yield start
        start = start + lens[d]


def own_starts(lens, offset, length):
    pos = offset + lax.broadcasted_iota(jnp.int32, (length, LANES), 0)
    found = jnp.zeros((length, LANES), jnp.int32)
    for start in starts_of(lens):
        found = jnp.where(pos >= start, start, found)
    return pos, found


def pair_of(cols, at):
    lane = lax.broadcasted_iota(jnp.int32, (cols.shape[0], LANES), 1)
    return jnp.where(lane < HEAD_SIZE, cols[:, at : at + 1], cols[:, at + 1 : at + 2])


def front_kernel(
    lens, offset_ref, x_ref, bc_ref, rim_ref, dt_ref, bias_ref, rate_ref, cw_ref, cb_ref, bw_ref, bb_ref,
    val_ref, kq_ref, cols_ref, rows_ref, e_ref, d_ref, xs, bs, rs,
):
    length, width = x_ref.shape
    heads = dt_ref.shape[0]
    offset = offset_ref[0]
    pos, found = own_starts(lens, offset, length)
    depth = pos - found
    last_start = jnp.int32(0)
    first_here = jnp.int32(2**30)
    for start in starts_of(lens):
        last_start = jnp.where(start <= offset + length - 1, start, last_start)
        first_here = jnp.where(start >= offset, jnp.minimum(first_here, start), first_here)

    bs[:RIM] = rim_ref[:, width:].astype(F32)
    bs[RIM:] = bc_ref[...].astype(F32)
    xs[:RIM] = rim_ref[:, :width].astype(F32)
    xs[RIM:] = x_ref[...].astype(F32)

    def conv(buf, w_ref, b_ref, at):
        sl = slice(at, at + LANES)
        total = jnp.zeros((length, LANES), F32) + b_ref[:, sl].astype(F32)
        for k in range(KERNEL):
            lag = KERNEL - 1 - k
            tap = w_ref[k : k + 1, sl].astype(F32) * buf[RIM - lag : RIM - lag + length, sl]
            total = total + (jnp.where(depth >= lag, tap, 0.0) if lag else tap)
        return silu(total).astype(BF16)

    for at in range(0, 2 * STATE, LANES):
        kq_ref[:, at : at + LANES] = conv(bs, bw_ref, bb_ref, at)

    head = lax.broadcasted_iota(jnp.int32, (heads, length), 0)

    def per_head(ref):
        spread = jnp.full((heads, length), ref[0], F32)
        for h in range(1, heads):
            spread = jnp.where(head == h, ref[h], spread)
        return spread

    raw = dt_ref[...] + per_head(bias_ref)
    steps = jnp.maximum(raw, 0.0) + jnp.log1p(jnp.exp(-jnp.abs(raw)))
    rates = steps * per_head(rate_ref)
    upper = (
        lax.broadcasted_iota(jnp.int32, (length, length), 0)
        <= lax.broadcasted_iota(jnp.int32, (length, length), 1)
    ).astype(F32).astype(BF16)
    high, middle, low = in_three(rates)
    climb = dot(low, upper) + dot(middle, upper) + dot(high, upper)
    end = climb[:, length - 1 :]
    spot = lax.broadcasted_iota(jnp.int32, (heads, length), 1)
    tail = jnp.where(spot >= last_start - offset, jnp.exp(climb - end) * steps, 0.0)
    entry = jnp.where(spot < first_here - offset, jnp.exp(-climb), 0.0)
    rs[...] = jnp.zeros(rs.shape, F32)
    rs[0:heads] = climb
    rs[16 : 16 + heads] = tail
    rs[32 : 32 + heads] = entry
    cols = rs[...].T
    cols_ref[...] = cols
    rows_ref[...] = jnp.zeros(rows_ref.shape, F32)
    rows_ref[0:heads] = climb
    rows_ref[16 : 16 + heads] = steps
    keys = kq_ref[:, :STATE].astype(F32).T.astype(BF16)
    for j in range(width // LANES):
        sl = slice(j * LANES, (j + 1) * LANES)
        value = conv(xs, cw_ref, cb_ref, j * LANES)
        val_ref[:, sl] = value
        high, low = in_two(value.astype(F32) * pair_of(cols, 16 + 2 * j))
        e_ref[:, sl] = dot(keys, high) + dot(keys, low)
        d_ref[:, sl] = pair_of(cols[length - 8 :], 32 + 2 * j)[7:8]


def intra_kernel(lens, offset_ref, kq_ref, val_ref, cols_ref, rows_ref, y_ref):
    length, width = val_ref.shape
    offset = offset_ref[0]
    _, found = own_starts(lens, offset, length)
    found = found - offset
    lane = lax.broadcasted_iota(jnp.int32, (LANES, LANES), 1)
    for i in range(length // LANES):
        rows = slice(i * LANES, (i + 1) * LANES)
        upto = (i + 1) * LANES
        scores = dot(kq_ref[rows, STATE:], kq_ref[:upto, :STATE], 1, 1)
        t = i * LANES + lax.broadcasted_iota(jnp.int32, (LANES, upto), 0)
        s = lax.broadcasted_iota(jnp.int32, (LANES, upto), 1)
        scores = jnp.where((s <= t) & (s >= found[rows, 0:1]), scores, 0.0)
        for j in range(width // LANES):
            sl = slice(j * LANES, (j + 1) * LANES)
            both = []
            for h in (2 * j, 2 * j + 1):
                gap = rows_ref[h : h + 1, :upto] - cols_ref[rows, h : h + 1]
                weight = jnp.exp(jnp.minimum(gap, 0.0)) * scores * rows_ref[16 + h : 17 + h, :upto]
                high, low = in_two(weight)
                both.append(dot(high, val_ref[:upto, sl]) + dot(low, val_ref[:upto, sl]))
            y_ref[rows, sl] = jnp.where(lane < HEAD_SIZE, both[0], both[1])


def gate_kernel(kq_ref, s_ref, cols_ref, y_ref, val_ref, z_ref, skip_ref, g0_ref, g1_ref, ss_ref):
    length, width = val_ref.shape
    half = length // 2
    cols = cols_ref[...]
    total = jnp.zeros((length, LANES), F32)
    for j in range(width // LANES):
        sl = slice(j * LANES, (j + 1) * LANES)
        high, low = in_two(s_ref[:, sl])
        far = dot(kq_ref[:, STATE:], high) + dot(kq_ref[:, STATE:], low)
        out = y_ref[:, sl] + far * pair_of(cols, 32 + 2 * j)
        mixed = out + skip_ref[:, sl] * val_ref[:, sl].astype(F32)
        gated = mixed * silu(z_ref[:, sl].astype(F32))
        g0_ref[:, sl] = gated[:half]
        g1_ref[:, sl] = gated[half:]
        total = total + gated * gated
    ss_ref[...] = jnp.sum(total.T, axis=0, keepdims=True)


def project_kernel(*refs, count, started, last):
    halves = refs[:count], refs[count : 2 * count]
    weights = refs[2 * count : 3 * count]
    rest, out_ref = refs[3 * count : -1], refs[-1]
    half = halves[0][0].shape[0]
    for k, pieces in enumerate(halves):
        sl = slice(k * half, (k + 1) * half)
        total = rest[0][:, sl] if started else None
        for piece, weight in zip(pieces, weights):
            part = dot(weight[...], piece[...], 1, 1)
            total = part if total is None else total + part
        out_ref[:, sl] = (rest[1][:, sl].astype(F32) + total).astype(BF16) if last else total


def logits_kernel(
    meta, *refs, overlap, width,
):
    pieces = refs[:16]
    gain_ref, target_ref, w_ref, out_ref, wide, hid, peak, total, pick, want = refs[16:]
    step = pl.program_id(0)
    block = w_ref.shape[1]
    depth = wide.shape[0]
    part, length = pieces[0].shape
    members = 2
    rows = members * length

    @pl.when(step == 0)
    def _():
        for m in range(members):
            squares = jnp.zeros((1, length), F32)
            for k in range(8):
                piece = pieces[4 * (k // 2) + 2 * m + k % 2][...]
                chip = (meta[2] + (0, 3, 1, 2)[k // 2]) % 4
                rank = 2 * chip + (1 - meta[3] if k % 2 else meta[3])
                wide[pl.ds(pl.multiple_of(rank * part, 64), part), :] = piece
                big = piece.astype(F32)
                squares = squares + jnp.sum(big * big, axis=0, keepdims=True)
            scale = lax.rsqrt(squares / depth + EPSILON)
            for at in range(0, depth, LANES):
                sl = slice(at, at + LANES)
                value = (wide[sl, :].astype(F32) * scale).T * gain_ref[:, sl].astype(F32)
                hid[m * length : (m + 1) * length, sl] = value.astype(BF16)
        want[...] = jnp.zeros((rows, LANES), jnp.int32) + target_ref[...]
        peak[...] = jnp.full((rows, LANES), NEG, F32)
        total[...] = jnp.zeros((rows, LANES), F32)
        pick[...] = jnp.zeros((rows, LANES), F32)

    logits = dot(hid[...], w_ref[...])
    lane = lax.broadcasted_iota(jnp.int32, (rows, LANES), 1)
    groups = []
    found = pick[...]
    old = peak[...]
    top = old
    for g in range(block // LANES):
        at = step * block + g * LANES
        good = ((meta[0] == 0) | (at >= overlap)) & (at < width)
        part = jnp.where(good, logits[:, g * LANES : (g + 1) * LANES], NEG)
        groups.append(part)
        found = found + jnp.where((lane + (at + meta[1]) == want[...]) & good, part, 0.0)
        top = jnp.maximum(top, part)
    add = total[...] * jnp.exp(old - top)
    for part in groups:
        add = add + jnp.exp(part - top)
    pick[...] = found
    peak[...] = top
    total[...] = add

    @pl.when(step == pl.num_programs(0) - 1)
    def _():
        tops = peak[...].T
        top = jnp.max(tops, axis=0, keepdims=True)
        out_ref[0:1, :] = top + jnp.log(jnp.sum(total[...].T * jnp.exp(tops - top), axis=0, keepdims=True))
        out_ref[1:2, :] = jnp.sum(pick[...].T, axis=0, keepdims=True)


def shape(dims, dtype):
    return jax.ShapeDtypeStruct(dims, dtype)


def cost(flops, nbytes):
    return pl.CostEstimate(flops=int(flops), bytes_accessed=int(nbytes), transcendentals=0)


def ring(length, by):
    return [(i, (i + by) % length) for i in range(length)]


def swapped(length, bit):
    return [(i, i ^ bit) for i in range(length)]


def from_chips(value, by):
    return lax.ppermute(value, "x", ring(lax.axis_size("x"), by))


def from_core(value):
    return lax.ppermute(value, "core", swapped(2, 1))


def summed_over_heads(value):
    value = value + from_core(value)
    return value + sum(from_chips(value, k) for k in range(1, lax.axis_size("x")))


def order_here():
    size = lax.axis_size("x")
    x, core = lax.axis_index("x"), lax.axis_index("core")
    spots = [x, x, x - 1, x - 1, x + 1, x + 1, x + 2, x + 2]
    return jnp.stack(
        [2 * lax.rem(s + size, size) + (1 - core if k % 2 else core) for k, s in enumerate(spots)]
    ).astype(jnp.int32)


def lse_of(parts):
    top = functools.reduce(jnp.maximum, [p[0:1] for p in parts])
    total = sum(jnp.exp(p[0:1] - top) for p in parts)
    return jnp.concatenate([top + jnp.log(total), sum(p[1:2] for p in parts)], axis=0)


def compute(
    residual, x_in, bc_in, z_in, dt_raw, dt_bias, decay_rate, d_skip, conv_x_weight, conv_x_bias,
    conv_bc_weight, conv_bc_bias, norm_gain, out_weight, final_gain, lm_weight, targets, doc_lengths,
):
    length, inner = x_in.shape
    ranks = lax.axis_size(HEADS_AXES)
    seq_size = lax.axis_size("seq")
    groups = lax.axis_size("groups")
    seq_rank = lax.axis_index("seq")
    head_rank = lax.axis_index(HEADS_AXES)
    parity = lax.rem(lax.axis_index("groups"), 2)
    mates = swapped(groups, 1)
    offset = (seq_rank * length).reshape(1).astype(jnp.int32)
    share = residual.shape[1]
    depth = share * ranks

    onward = [(i, i + 1) for i in range(seq_size - 1)]
    rim = jnp.concatenate([x_in[length - RIM :], bc_in[length - RIM :]], axis=1)
    rim = lax.ppermute(rim, "seq", onward)

    values, kq, cols, rows, state, through = pl.pallas_call(
        front_kernel,
        out_shape=(
            shape((length, inner), BF16),
            shape((length, 2 * STATE), BF16),
            shape((length, LANES), F32),
            shape((32, length), F32),
            shape((STATE, inner), F32),
            shape((1, inner), F32),
        ),
        in_specs=[SMEM, SMEM] + [pl.BlockSpec()] * 4 + [SMEM, SMEM] + [pl.BlockSpec()] * 4,
        scratch_shapes=[
            pltpu.VMEM((length + RIM, inner), F32),
            pltpu.VMEM((length + RIM, 2 * STATE), F32),
            pltpu.VMEM((LANES, length), F32),
        ],
        name="front",
    )(
        doc_lengths, offset, x_in, bc_in, rim, dt_raw, dt_bias, decay_rate,
        conv_x_weight, conv_x_bias[None], conv_bc_weight, conv_bc_bias[None],
    )

    incoming = lax.ppermute(state, "seq", onward)
    through, out_weight, targets, d_skip = lax.optimization_barrier((through, out_weight, targets, d_skip))
    for n in range(2, -(-(LONGEST - 1) // length) + 1):
        carried = state + through * incoming
        incoming = lax.ppermute(carried, "seq", onward)
        if n == 2:
            incoming, lm_weight = lax.optimization_barrier((incoming, lm_weight))

    vocab = lm_weight.shape[1]
    block = 256
    width = -(-vocab // (2 * LANES)) * LANES
    overlap = 2 * width - vocab
    first_column = parity * (vocab - width)
    mine = lax.dynamic_slice_in_dim(lm_weight, first_column, width, 1)
    embedding = lax.all_gather(mine, "seq", axis=0, tiled=True)

    order = order_here()
    meta = jnp.stack([parity, first_column, lax.axis_index("x"), lax.axis_index("core")]).astype(jnp.int32)
    their_targets = lax.ppermute(targets, "groups", mates)
    wanted = (jnp.concatenate([targets, their_targets]) - head_rank * vocab)[:, None]
    skip = jnp.repeat(d_skip, HEAD_SIZE)[None]
    turned = out_weight.T.reshape(ranks, share, inner)
    weights = lax.all_to_all(turned, HEADS_AXES, 0, 0, tiled=True)

    inside = pl.pallas_call(
        intra_kernel,
        out_shape=shape((length, inner), F32),
        in_specs=[SMEM, SMEM] + [pl.BlockSpec()] * 4,
        cost_estimate=cost(5e9, 4e6),
        name="intra",
    )(doc_lengths, offset, kq, values, cols, rows)
    by_rank = [lax.dynamic_index_in_dim(weights, order[k], 0, False) for k in range(ranks)]
    incoming, meta, wanted, skip = lax.optimization_barrier((incoming, meta, wanted, skip))

    half = length // 2
    gated0, gated1, squares = pl.pallas_call(
        gate_kernel,
        out_shape=(shape((half, inner), F32), shape((half, inner), F32), shape((1, length), F32)),
        name="gate",
    )(kq, incoming, cols, inside, values, z_in, skip)
    squares = summed_over_heads(squares)
    scale = lax.rsqrt(squares[0] / (inner * ranks) + EPSILON)[:, None]
    gain = norm_gain.astype(F32)[None, :]
    low = (gated0 * scale[:half] * gain).astype(BF16)
    high = (gated1 * scale[half:] * gain).astype(BF16)

    def project(lows, highs, weights, *rest, last=False):
        return pl.pallas_call(
            functools.partial(project_kernel, count=len(lows), started=len(rest) > 0, last=last),
            out_shape=shape((share, length), BF16 if last else F32),
            cost_estimate=cost(3e9, 4e6),
            name="project",
        )(*lows, *highs, *weights, *rest)

    left_low, right_high = from_chips(low, 1), from_chips(high, -1)
    left_high, right_low = from_chips(high, 1), from_chips(low, -1)
    low_other, high_other = from_core(low), from_core(high)
    projected = project((low, low_other), (high, high_other), by_rank[:2])
    far_low, far_high = from_chips(left_low, 1), from_chips(right_high, -1)
    left_low_other, right_high_other = from_core(left_low), from_core(right_high)
    left_high_other, right_low_other = from_core(left_high), from_core(right_low)
    projected = project(
        (left_low, left_low_other, right_low, right_low_other),
        (left_high, left_high_other, right_high, right_high_other),
        by_rank[2:6],
        projected,
    )
    far_low, far_high, projected = lax.optimization_barrier((far_low, far_high, projected))
    block_out = project(
        (far_low, from_core(far_low)), (far_high, from_core(far_high)), by_rank[6:8],
        projected, residual.T, last=True,
    )

    own1 = lax.ppermute(block_out, "groups", mates)
    own0 = block_out
    left0, right0 = from_chips(own0, 1), from_chips(own0, -1)
    left1, right1 = from_chips(own1, 1), from_chips(own1, -1)
    far0 = from_chips(left0, 1)
    far1 = from_chips(right1, -1)
    mine = (own0, own1, left0, left1, right0, right1, far0, far1)
    pieces = [p for own in mine for p in (own, from_core(own))]
    whole = pl.BlockSpec()
    losses = pl.pallas_call(
        functools.partial(logits_kernel, overlap=overlap, width=width),
        out_shape=shape((2, 2 * length), F32),
        grid=(-(-width // block),),
        in_specs=[SMEM] + [whole] * 18 + [pl.BlockSpec((depth, block), lambda i: (0, i))],
        out_specs=pl.BlockSpec((2, 2 * length), lambda i: (0, 0)),
        scratch_shapes=[
            pltpu.VMEM((depth, length), BF16),
            pltpu.VMEM((2 * length, depth), BF16),
            pltpu.VMEM((2 * length, LANES), F32),
            pltpu.VMEM((2 * length, LANES), F32),
            pltpu.VMEM((2 * length, LANES), F32),
            pltpu.VMEM((2 * length, LANES), jnp.int32),
        ],
        name="logits",
    )(
        meta, *pieces, final_gain[None], wanted, embedding,
    )

    mine, given = losses[:, :length], losses[:, length:]
    axes = ("groups", "core")
    across = [(2 * g + c, 2 * (g ^ 1) + (c ^ 1)) for g in range(groups) for c in range(2)]
    parts = lse_of(
        [mine, from_core(mine), lax.ppermute(given, "groups", mates), lax.ppermute(given, axes, across)]
    )
    parts = lse_of([parts] + [from_chips(parts, k) for k in range(1, lax.axis_size("x"))])
    tokens = (parts[0:1] - parts[1:2])[0]

    ends = jnp.cumsum(doc_lengths)
    positions = offset[0] + jnp.arange(length, dtype=jnp.int32)
    member = (positions[:, None] < ends[None, :]) & (positions[:, None] >= (ends - doc_lengths)[None, :])
    sums = jnp.sum(jnp.where(member, tokens[:, None], 0.0), axis=0)
    everyone = jnp.broadcast_to(sums[None, None], (seq_size, 1, sums.shape[0]))
    sums = lax.all_to_all(everyone, "seq", 0, 0, tiled=True).sum(axis=(0, 1))
    return block_out.T, sums / doc_lengths.astype(F32)


def solution(mesh):
    groups, seq, head = (mesh.shape[name] for name in ("groups", "seq", "head"))
    split = Mesh(mesh.devices.reshape(groups, seq, head // 2, 2), ("groups", "seq", "x", "core"))
    tokens = ("groups", "seq")
    heads = HEADS_AXES
    in_specs = (
        P(tokens, heads), P(tokens, heads), P(tokens, None), P(tokens, heads), P(heads, tokens),
        P(heads), P(heads), P(heads), P(None, heads), P(heads), P(), P(), P(heads), P(heads, None),
        P(), P("seq", heads), P(tokens), P("groups"),
    )
    out_specs = (P(tokens, heads), P("groups"))
    return jax.shard_map(compute, mesh=split, in_specs=in_specs, out_specs=out_specs, check_vma=False)
```

```python
import functools

import jax
import jax.numpy as jnp
from jax import lax
from jax.experimental import pallas as pl
from jax.experimental.pallas import tpu as pltpu
from jax.sharding import Mesh
from jax.sharding import PartitionSpec as P


STATE = 128
HEAD_SIZE = 64
KERNEL = 4
LONGEST = 1536
EPSILON = 1e-05
LANES = 128
RIM = 8
NEG = -1e30
F32 = jnp.float32
BF16 = jnp.bfloat16

SMEM = pl.BlockSpec(memory_space=pltpu.SMEM)
HEADS_AXES = ("x", "core")


def dot(a, b, ca=1, cb=0):
    return lax.dot_general(a, b, (((ca,), (cb,)), ((), ())), preferred_element_type=F32)


def in_two(value):
    high = value.astype(BF16)
    return high, (value - high.astype(F32)).astype(BF16)


def in_three(value):
    high = value.astype(BF16)
    rest = value - high.astype(F32)
    middle = rest.astype(BF16)
    return high, middle, (rest - middle.astype(F32)).astype(BF16)


def silu(value):
    return value * jax.nn.sigmoid(value)


def starts_of(lens):
    start = jnp.int32(0)
    for d in range(lens.shape[0]):
        yield start
        start = start + lens[d]


def own_starts(lens, offset, length):
    pos = offset + lax.broadcasted_iota(jnp.int32, (length, LANES), 0)
    found = jnp.zeros((length, LANES), jnp.int32)
    for start in starts_of(lens):
        found = jnp.where(pos >= start, start, found)
    return pos, found


def pair_of(cols, at):
    lane = lax.broadcasted_iota(jnp.int32, (cols.shape[0], LANES), 1)
    return jnp.where(lane < HEAD_SIZE, cols[:, at : at + 1], cols[:, at + 1 : at + 2])


def front_kernel(
    lens, offset_ref, x_ref, bc_ref, rim_ref, dt_ref, bias_ref, rate_ref, cw_ref, cb_ref, bw_ref, bb_ref,
    val_ref, kq_ref, cols_ref, rows_ref, e_ref, d_ref, xs, bs, rs,
):
    length, width = x_ref.shape
    heads = dt_ref.shape[0]
    offset = offset_ref[0]
    pos, found = own_starts(lens, offset, length)
    depth = pos - found
    last_start = jnp.int32(0)
    first_here = jnp.int32(2**30)
    for start in starts_of(lens):
        last_start = jnp.where(start <= offset + length - 1, start, last_start)
        first_here = jnp.where(start >= offset, jnp.minimum(first_here, start), first_here)

    bs[:RIM] = rim_ref[:, width:].astype(F32)
    bs[RIM:] = bc_ref[...].astype(F32)
    xs[:RIM] = rim_ref[:, :width].astype(F32)
    xs[RIM:] = x_ref[...].astype(F32)

    def conv(buf, w_ref, b_ref, at):
        sl = slice(at, at + LANES)
        total = jnp.zeros((length, LANES), F32) + b_ref[:, sl].astype(F32)
        for k in range(KERNEL):
            lag = KERNEL - 1 - k
            tap = w_ref[k : k + 1, sl].astype(F32) * buf[RIM - lag : RIM - lag + length, sl]
            total = total + (jnp.where(depth >= lag, tap, 0.0) if lag else tap)
        return silu(total).astype(BF16)

    for at in range(0, 2 * STATE, LANES):
        kq_ref[:, at : at + LANES] = conv(bs, bw_ref, bb_ref, at)

    head = lax.broadcasted_iota(jnp.int32, (heads, length), 0)

    def per_head(ref):
        spread = jnp.full((heads, length), ref[0], F32)
        for h in range(1, heads):
            spread = jnp.where(head == h, ref[h], spread)
        return spread

    raw = dt_ref[...] + per_head(bias_ref)
    steps = jnp.maximum(raw, 0.0) + jnp.log1p(jnp.exp(-jnp.abs(raw)))
    rates = steps * per_head(rate_ref)
    upper = (
        lax.broadcasted_iota(jnp.int32, (length, length), 0)
        <= lax.broadcasted_iota(jnp.int32, (length, length), 1)
    ).astype(F32).astype(BF16)
    high, middle, low = in_three(rates)
    climb = dot(low, upper) + dot(middle, upper) + dot(high, upper)
    end = climb[:, length - 1 :]
    spot = lax.broadcasted_iota(jnp.int32, (heads, length), 1)
    tail = jnp.where(spot >= last_start - offset, jnp.exp(climb - end) * steps, 0.0)
    entry = jnp.where(spot < first_here - offset, jnp.exp(-climb), 0.0)
    rs[...] = jnp.zeros(rs.shape, F32)
    rs[0:heads] = climb
    rs[16 : 16 + heads] = tail
    rs[32 : 32 + heads] = entry
    cols = rs[...].T
    cols_ref[...] = cols
    rows_ref[...] = jnp.zeros(rows_ref.shape, F32)
    rows_ref[0:heads] = climb
    rows_ref[16 : 16 + heads] = steps
    keys = kq_ref[:, :STATE].astype(F32).T.astype(BF16)
    for j in range(width // LANES):
        sl = slice(j * LANES, (j + 1) * LANES)
        value = conv(xs, cw_ref, cb_ref, j * LANES)
        val_ref[:, sl] = value
        high, low = in_two(value.astype(F32) * pair_of(cols, 16 + 2 * j))
        e_ref[:, sl] = dot(keys, high) + dot(keys, low)
        d_ref[:, sl] = pair_of(cols[length - 8 :], 32 + 2 * j)[7:8]


def intra_kernel(lens, offset_ref, kq_ref, val_ref, cols_ref, rows_ref, y_ref):
    length, width = val_ref.shape
    offset = offset_ref[0]
    _, found = own_starts(lens, offset, length)
    found = found - offset
    lane = lax.broadcasted_iota(jnp.int32, (LANES, LANES), 1)
    for i in range(length // LANES):
        rows = slice(i * LANES, (i + 1) * LANES)
        upto = (i + 1) * LANES
        scores = dot(kq_ref[rows, STATE:], kq_ref[:upto, :STATE], 1, 1)
        t = i * LANES + lax.broadcasted_iota(jnp.int32, (LANES, upto), 0)
        s = lax.broadcasted_iota(jnp.int32, (LANES, upto), 1)
        scores = jnp.where((s <= t) & (s >= found[rows, 0:1]), scores, 0.0)
        for j in range(width // LANES):
            sl = slice(j * LANES, (j + 1) * LANES)
            both = []
            for h in (2 * j, 2 * j + 1):
                gap = rows_ref[h : h + 1, :upto] - cols_ref[rows, h : h + 1]
                weight = jnp.exp(jnp.minimum(gap, 0.0)) * scores * rows_ref[16 + h : 17 + h, :upto]
                high, low = in_two(weight)
                both.append(dot(high, val_ref[:upto, sl]) + dot(low, val_ref[:upto, sl]))
            y_ref[rows, sl] = jnp.where(lane < HEAD_SIZE, both[0], both[1])


def gate_kernel(kq_ref, s_ref, cols_ref, y_ref, val_ref, z_ref, skip_ref, g0_ref, g1_ref, ss_ref):
    length, width = val_ref.shape
    half = length // 2
    cols = cols_ref[...]
    total = jnp.zeros((length, LANES), F32)
    for j in range(width // LANES):
        sl = slice(j * LANES, (j + 1) * LANES)
        high, low = in_two(s_ref[:, sl])
        far = dot(kq_ref[:, STATE:], high) + dot(kq_ref[:, STATE:], low)
        out = y_ref[:, sl] + far * pair_of(cols, 32 + 2 * j)
        mixed = out + skip_ref[:, sl] * val_ref[:, sl].astype(F32)
        gated = mixed * silu(z_ref[:, sl].astype(F32))
        g0_ref[:, sl] = gated[:half]
        g1_ref[:, sl] = gated[half:]
        total = total + gated * gated
    ss_ref[...] = jnp.sum(total.T, axis=0, keepdims=True)


def project_kernel(*refs, count, started, last):
    halves = refs[:count], refs[count : 2 * count]
    weights = refs[2 * count : 3 * count]
    rest, out_ref = refs[3 * count : -1], refs[-1]
    half = halves[0][0].shape[0]
    for k, pieces in enumerate(halves):
        sl = slice(k * half, (k + 1) * half)
        total = rest[0][:, sl] if started else None
        for piece, weight in zip(pieces, weights):
            part = dot(weight[...], piece[...], 1, 1)
            total = part if total is None else total + part
        out_ref[:, sl] = (rest[1][:, sl].astype(F32) + total).astype(BF16) if last else total


def logits_kernel(
    meta, *refs, overlap, width,
):
    pieces = refs[:16]
    gain_ref, target_ref, w_ref, out_ref, wide, hid, peak, total, pick, want = refs[16:]
    step = pl.program_id(0)
    block = w_ref.shape[1]
    depth = wide.shape[0]
    part, length = pieces[0].shape
    members = 2
    rows = members * length

    @pl.when(step == 0)
    def _():
        for m in range(members):
            squares = jnp.zeros((1, length), F32)
            for k in range(8):
                piece = pieces[4 * (k // 2) + 2 * m + k % 2][...]
                chip = (meta[2] + (0, 3, 1, 2)[k // 2]) % 4
                rank = 2 * chip + (1 - meta[3] if k % 2 else meta[3])
                wide[pl.ds(pl.multiple_of(rank * part, 64), part), :] = piece
                big = piece.astype(F32)
                squares = squares + jnp.sum(big * big, axis=0, keepdims=True)
            scale = lax.rsqrt(squares / depth + EPSILON)
            for at in range(0, depth, LANES):
                sl = slice(at, at + LANES)
                value = (wide[sl, :].astype(F32) * scale).T * gain_ref[:, sl].astype(F32)
                hid[m * length : (m + 1) * length, sl] = value.astype(BF16)
        want[...] = jnp.zeros((rows, LANES), jnp.int32) + target_ref[...]
        peak[...] = jnp.full((rows, LANES), NEG, F32)
        total[...] = jnp.zeros((rows, LANES), F32)
        pick[...] = jnp.zeros((rows, LANES), F32)

    logits = dot(hid[...], w_ref[...])
    lane = lax.broadcasted_iota(jnp.int32, (rows, LANES), 1)
    groups = []
    found = pick[...]
    old = peak[...]
    top = old
    for g in range(block // LANES):
        at = step * block + g * LANES
        good = ((meta[0] == 0) | (at >= overlap)) & (at < width)
        part = jnp.where(good, logits[:, g * LANES : (g + 1) * LANES], NEG)
        groups.append(part)
        found = found + jnp.where((lane + (at + meta[1]) == want[...]) & good, part, 0.0)
        top = jnp.maximum(top, part)
    add = total[...] * jnp.exp(old - top)
    for part in groups:
        add = add + jnp.exp(part - top)
    pick[...] = found
    peak[...] = top
    total[...] = add

    @pl.when(step == pl.num_programs(0) - 1)
    def _():
        tops = peak[...].T
        top = jnp.max(tops, axis=0, keepdims=True)
        out_ref[0:1, :] = top + jnp.log(jnp.sum(total[...].T * jnp.exp(tops - top), axis=0, keepdims=True))
        out_ref[1:2, :] = jnp.sum(pick[...].T, axis=0, keepdims=True)


def shape(dims, dtype):
    return jax.ShapeDtypeStruct(dims, dtype)


def cost(flops, nbytes):
    return pl.CostEstimate(flops=int(flops), bytes_accessed=int(nbytes), transcendentals=0)


def ring(length, by):
    return [(i, (i + by) % length) for i in range(length)]


def swapped(length, bit):
    return [(i, i ^ bit) for i in range(length)]


def from_chips(value, by):
    return lax.ppermute(value, "x", ring(lax.axis_size("x"), by))


def from_core(value):
    return lax.ppermute(value, "core", swapped(2, 1))


def summed_over_heads(value):
    value = value + from_core(value)
    return value + sum(from_chips(value, k) for k in range(1, lax.axis_size("x")))


def order_here():
    size = lax.axis_size("x")
    x, core = lax.axis_index("x"), lax.axis_index("core")
    spots = [x, x, x - 1, x - 1, x + 1, x + 1, x + 2, x + 2]
    return jnp.stack(
        [2 * lax.rem(s + size, size) + (1 - core if k % 2 else core) for k, s in enumerate(spots)]
    ).astype(jnp.int32)


def lse_of(parts):
    top = functools.reduce(jnp.maximum, [p[0:1] for p in parts])
    total = sum(jnp.exp(p[0:1] - top) for p in parts)
    return jnp.concatenate([top + jnp.log(total), sum(p[1:2] for p in parts)], axis=0)


def compute(
    residual, x_in, bc_in, z_in, dt_raw, dt_bias, decay_rate, d_skip, conv_x_weight, conv_x_bias,
    conv_bc_weight, conv_bc_bias, norm_gain, out_weight, final_gain, lm_weight, targets, doc_lengths,
):
    length, inner = x_in.shape
    ranks = lax.axis_size(HEADS_AXES)
    seq_size = lax.axis_size("seq")
    groups = lax.axis_size("groups")
    seq_rank = lax.axis_index("seq")
    head_rank = lax.axis_index(HEADS_AXES)
    parity = lax.rem(lax.axis_index("groups"), 2)
    mates = swapped(groups, 1)
    offset = (seq_rank * length).reshape(1).astype(jnp.int32)
    share = residual.shape[1]
    depth = share * ranks

    onward = [(i, i + 1) for i in range(seq_size - 1)]
    rim = jnp.concatenate([x_in[length - RIM :], bc_in[length - RIM :]], axis=1)
    rim = lax.ppermute(rim, "seq", onward)

    values, kq, cols, rows, state, through = pl.pallas_call(
        front_kernel,
        out_shape=(
            shape((length, inner), BF16),
            shape((length, 2 * STATE), BF16),
            shape((length, LANES), F32),
            shape((32, length), F32),
            shape((STATE, inner), F32),
            shape((1, inner), F32),
        ),
        in_specs=[SMEM, SMEM] + [pl.BlockSpec()] * 4 + [SMEM, SMEM] + [pl.BlockSpec()] * 4,
        scratch_shapes=[
            pltpu.VMEM((length + RIM, inner), F32),
            pltpu.VMEM((length + RIM, 2 * STATE), F32),
            pltpu.VMEM((LANES, length), F32),
        ],
        name="front",
    )(
        doc_lengths, offset, x_in, bc_in, rim, dt_raw, dt_bias, decay_rate,
        conv_x_weight, conv_x_bias[None], conv_bc_weight, conv_bc_bias[None],
    )

    incoming = lax.ppermute(state, "seq", onward)
    through, out_weight, lm_weight = lax.optimization_barrier((through, out_weight, lm_weight))
    vocab = lm_weight.shape[1]
    block = 256
    width = -(-vocab // (2 * LANES)) * LANES
    overlap = 2 * width - vocab
    first_column = parity * (vocab - width)
    mine = lax.dynamic_slice_in_dim(lm_weight, first_column, width, 1)
    incoming, mine = lax.optimization_barrier((incoming, mine))
    for n in range(2, -(-(LONGEST - 1) // length) + 1):
        carried = state + through * incoming
        incoming = lax.ppermute(carried, "seq", onward)
        if n == 2:
            incoming, targets, d_skip, parity = lax.optimization_barrier((incoming, targets, d_skip, parity))

    embedding = lax.all_gather(mine, "seq", axis=0, tiled=True)

    order = order_here()
    meta = jnp.stack([parity, first_column, lax.axis_index("x"), lax.axis_index("core")]).astype(jnp.int32)
    their_targets = lax.ppermute(targets, "groups", mates)
    wanted = (jnp.concatenate([targets, their_targets]) - head_rank * vocab)[:, None]
    skip = jnp.repeat(d_skip, HEAD_SIZE)[None]
    turned = out_weight.T.reshape(ranks, share, inner)
    weights = lax.all_to_all(turned, HEADS_AXES, 0, 0, tiled=True)

    inside = pl.pallas_call(
        intra_kernel,
        out_shape=shape((length, inner), F32),
        in_specs=[SMEM, SMEM] + [pl.BlockSpec()] * 4,
        cost_estimate=cost(5e9, 4e6),
        name="intra",
    )(doc_lengths, offset, kq, values, cols, rows)
    by_rank = [lax.dynamic_index_in_dim(weights, order[k], 0, False) for k in range(ranks)]
    incoming, meta, wanted, skip = lax.optimization_barrier((incoming, meta, wanted, skip))

    half = length // 2
    gated0, gated1, squares = pl.pallas_call(
        gate_kernel,
        out_shape=(shape((half, inner), F32), shape((half, inner), F32), shape((1, length), F32)),
        name="gate",
    )(kq, incoming, cols, inside, values, z_in, skip)
    squares = summed_over_heads(squares)
    scale = lax.rsqrt(squares[0] / (inner * ranks) + EPSILON)[:, None]
    gain = norm_gain.astype(F32)[None, :]
    low = (gated0 * scale[:half] * gain).astype(BF16)
    high = (gated1 * scale[half:] * gain).astype(BF16)

    def project(lows, highs, weights, *rest, last=False):
        return pl.pallas_call(
            functools.partial(project_kernel, count=len(lows), started=len(rest) > 0, last=last),
            out_shape=shape((share, length), BF16 if last else F32),
            cost_estimate=cost(3e9, 4e6),
            name="project",
        )(*lows, *highs, *weights, *rest)

    left_low, right_high = from_chips(low, 1), from_chips(high, -1)
    left_high, right_low = from_chips(high, 1), from_chips(low, -1)
    low_other, high_other = from_core(low), from_core(high)
    projected = project((low, low_other), (high, high_other), by_rank[:2])
    far_low, far_high = from_chips(left_low, 1), from_chips(right_high, -1)
    left_low_other, right_high_other = from_core(left_low), from_core(right_high)
    left_high_other, right_low_other = from_core(left_high), from_core(right_low)
    projected = project(
        (left_low, left_low_other, right_low, right_low_other),
        (left_high, left_high_other, right_high, right_high_other),
        by_rank[2:6],
        projected,
    )
    far_low, far_high, projected = lax.optimization_barrier((far_low, far_high, projected))
    block_out = project(
        (far_low, from_core(far_low)), (far_high, from_core(far_high)), by_rank[6:8],
        projected, residual.T, last=True,
    )

    own1 = lax.ppermute(block_out, "groups", mates)
    own0 = block_out
    left0, right0 = from_chips(own0, 1), from_chips(own0, -1)
    left1, right1 = from_chips(own1, 1), from_chips(own1, -1)
    far0 = from_chips(left0, 1)
    far1 = from_chips(right1, -1)
    mine = (own0, own1, left0, left1, right0, right1, far0, far1)
    pieces = [p for own in mine for p in (own, from_core(own))]
    whole = pl.BlockSpec()
    losses = pl.pallas_call(
        functools.partial(logits_kernel, overlap=overlap, width=width),
        out_shape=shape((2, 2 * length), F32),
        grid=(-(-width // block),),
        in_specs=[SMEM] + [whole] * 18 + [pl.BlockSpec((depth, block), lambda i: (0, i))],
        out_specs=pl.BlockSpec((2, 2 * length), lambda i: (0, 0)),
        scratch_shapes=[
            pltpu.VMEM((depth, length), BF16),
            pltpu.VMEM((2 * length, depth), BF16),
            pltpu.VMEM((2 * length, LANES), F32),
            pltpu.VMEM((2 * length, LANES), F32),
            pltpu.VMEM((2 * length, LANES), F32),
            pltpu.VMEM((2 * length, LANES), jnp.int32),
        ],
        name="logits",
    )(
        meta, *pieces, final_gain[None], wanted, embedding,
    )

    mine, given = losses[:, :length], losses[:, length:]
    axes = ("groups", "core")
    across = [(2 * g + c, 2 * (g ^ 1) + (c ^ 1)) for g in range(groups) for c in range(2)]
    parts = lse_of(
        [mine, from_core(mine), lax.ppermute(given, "groups", mates), lax.ppermute(given, axes, across)]
    )
    parts = lse_of([parts] + [from_chips(parts, k) for k in range(1, lax.axis_size("x"))])
    tokens = (parts[0:1] - parts[1:2])[0]

    ends = jnp.cumsum(doc_lengths)
    positions = offset[0] + jnp.arange(length, dtype=jnp.int32)
    member = (positions[:, None] < ends[None, :]) & (positions[:, None] >= (ends - doc_lengths)[None, :])
    sums = jnp.sum(jnp.where(member, tokens[:, None], 0.0), axis=0)
    everyone = jnp.broadcast_to(sums[None, None], (seq_size, 1, sums.shape[0]))
    sums = lax.all_to_all(everyone, "seq", 0, 0, tiled=True).sum(axis=(0, 1))
    return block_out.T, sums / doc_lengths.astype(F32)


def solution(mesh):
    groups, seq, head = (mesh.shape[name] for name in ("groups", "seq", "head"))
    split = Mesh(mesh.devices.reshape(groups, seq, head // 2, 2), ("groups", "seq", "x", "core"))
    tokens = ("groups", "seq")
    heads = HEADS_AXES
    in_specs = (
        P(tokens, heads), P(tokens, heads), P(tokens, None), P(tokens, heads), P(heads, tokens),
        P(heads), P(heads), P(heads), P(None, heads), P(heads), P(), P(), P(heads), P(heads, None),
        P(), P("seq", heads), P(tokens), P("groups"),
    )
    out_specs = (P(tokens, heads), P("groups"))
    return jax.shard_map(compute, mesh=split, in_specs=in_specs, out_specs=out_specs, check_vma=False)
```
